1024 devices in a mesh: ctx: 128 (over z, x), tp: 8 (over y, core).
Axes of the slice: x: 4, y: 4, z: 32, core: 2. Of those that a mesh axis runs over, the one named last changes fastest.
Arguments:
- queries: bfloat16 [32768, 8192], P(('ctx', 'tp')), may hold values from -6 to 6
- keys: bfloat16 [32768, 1024], P(('ctx', 'tp')), may hold values from -6 to 6
- values: bfloat16 [32768, 1024], P(('ctx', 'tp')), may hold values from -6 to 6
- doc_starts: int32 [77], replicated, may hold values from 0 to 32768, as said below
Outputs:
- attended: bfloat16 [32768, 8192], P(('ctx', 'tp'))
The draws below stay inside these ranges and needn't reach their ends.
Inputs may be any that keep to these rules, and one draw needn't show every extreme that they name: `doc_starts`: nondecreasing and starting with 0; consecutive entries differ by at most 1792, and some pair of consecutive entries below 32768 differs by exactly 1792; the last document ends at 32768, and entries equal to 32768 stand for empty documents.
All inputs are finite; a program needn't handle non-finite values.
Results may differ from the reference program's by a relative error of at most 0.004.
Values may be sent and summed in bfloat16 or wider, within the bound.
No kernel may reach another device: no remote copies, remote signals or barrier semaphores. Data moves between devices by JAX's collectives and lax.ppermute only.
A program may use at most 32 MiB of HBM per device.

```python
import jax
import jax.numpy as jnp
from jax import lax

QUERY_HEAD_COUNT = 64
KEY_VALUE_HEADS = 8
HEAD_WIDTH = 128
TOK_DEV = 32
PACKED_TOKENS = 32768
MOST = 1792
NDOCS = 77
N_CTX = 128
N_TP = 8


def draw_queries(key, part):
    start_offset = jnp.clip(jax.random.normal(jax.random.fold_in(key, 1), (PACKED_TOKENS, QUERY_HEAD_COUNT * HEAD_WIDTH), jnp.float32), -5.0, 5.0)
    return start_offset.astype(jnp.bfloat16)


def draw_keys(key, part):
    start_offset = jnp.clip(jax.random.normal(jax.random.fold_in(key, 2), (PACKED_TOKENS, KEY_VALUE_HEADS * HEAD_WIDTH), jnp.float32), -5.0, 5.0)
    return start_offset.astype(jnp.bfloat16)


def draw_doc_starts(key, part):
    lowest = MOST // 4
    spread = MOST - lowest
    first_draw = jax.random.randint(jax.random.fold_in(key, 21), (NDOCS,), 0, spread + 1, dtype=jnp.int32)
    second_draw = jax.random.randint(jax.random.fold_in(key, 22), (NDOCS,), 0, spread + 1, dtype=jnp.int32)
    lengths = lowest + first_draw * second_draw // spread
    chosen = jax.random.randint(jax.random.fold_in(key, 23), (), 0, PACKED_TOKENS // MOST - 1, dtype=jnp.int32)
    lengths = jnp.where(jnp.arange(NDOCS, dtype=jnp.int32) == chosen, MOST, lengths).astype(jnp.int32)
    ends = jnp.cumsum(lengths).astype(jnp.int32)
    starts = jnp.concatenate([jnp.zeros((1,), jnp.int32), ends[:-1]])
    return jnp.minimum(starts, PACKED_TOKENS).astype(jnp.int32)


def levels(key, extent, pieces, smallest, high):
    loudness = 1.0
    for axis_at, parts in pieces:
        heights = jax.random.uniform(jax.random.fold_in(jax.random.fold_in(key, 6), axis_at), (parts,), jnp.float32, smallest / len(pieces), high / len(pieces))
        loudness = loudness * jnp.repeat(jnp.exp(heights), extent[axis_at] // parts).reshape((-1,) + (1,) * (len(extent) - 1 - axis_at))
    return loudness


def normal_values(stream_key, extent, scale, reach, cuts=(), held_as=jnp.bfloat16):
    entries = jax.random.normal(stream_key, extent, jnp.float32) * scale
    if len(cuts) > 0:
        entries = levels(stream_key, extent, cuts, -0.22, 0.18) * entries
    return jnp.clip(entries, min=-reach, max=reach).astype(held_as)


def setup_inputs(seed: int = 0) -> dict:
    arg_keys = jax.random.split(jax.random.key(seed), 5)
    queries = draw_queries(jax.random.fold_in(arg_keys[4], 71), 0)
    keys = draw_keys(jax.random.fold_in(arg_keys[4], 71), 0)
    values = normal_values(arg_keys[2], (PACKED_TOKENS, KEY_VALUE_HEADS * HEAD_WIDTH), 1.0, 6.0, ((0, 1024),))
    doc_starts = draw_doc_starts(jax.random.fold_in(arg_keys[4], 71), 0)
    return dict(queries=queries, keys=keys, values=values, doc_starts=doc_starts)


def doc_begin(positions, doc_starts):
    found = jnp.where(doc_starts[None, :] <= positions[:, None], doc_starts[None, :], 0)
    return jnp.max(found, axis=1)


def reference(queries, keys, values, doc_starts):
    rows_per_block = TOK_DEV * N_TP
    reach_blocks = min(8, N_CTX // 2)
    visible_span = reach_blocks * rows_per_block
    query_groups = QUERY_HEAD_COUNT // KEY_VALUE_HEADS
    scale = HEAD_WIDTH ** -0.5
    leading_count = (reach_blocks - 1) * rows_per_block
    padded_key_rows = jnp.concatenate([jnp.zeros((leading_count, KEY_VALUE_HEADS * HEAD_WIDTH), jnp.bfloat16), keys], axis=0)
    padded_value_rows = jnp.concatenate([jnp.zeros((leading_count, KEY_VALUE_HEADS * HEAD_WIDTH), jnp.bfloat16), values], axis=0)

    def one_block(index):
        leading_entry = (index * rows_per_block).astype(jnp.int32)
        query_matrix = lax.dynamic_slice_in_dim(queries, leading_entry, rows_per_block, 0)
        query_matrix = query_matrix.reshape(rows_per_block, KEY_VALUE_HEADS, query_groups, HEAD_WIDTH).astype(jnp.float32)
        key_matrix = lax.dynamic_slice_in_dim(padded_key_rows, leading_entry, visible_span, 0).reshape(visible_span, KEY_VALUE_HEADS, HEAD_WIDTH).astype(jnp.float32)
        value_matrix = lax.dynamic_slice_in_dim(padded_value_rows, leading_entry, visible_span, 0).reshape(visible_span, KEY_VALUE_HEADS, HEAD_WIDTH).astype(jnp.float32)
        scores = jnp.einsum("qkgd,pkd->kgqp", query_matrix, key_matrix) * scale
        query_pos = leading_entry + jnp.arange(rows_per_block, dtype=jnp.int32)
        key_pos = leading_entry - leading_count + jnp.arange(visible_span, dtype=jnp.int32)
        begins = doc_begin(query_pos, doc_starts)
        visible = (key_pos[None, :] <= query_pos[:, None]) & (key_pos[None, :] >= begins[:, None])
        scores = jnp.where(visible, scores, -1e30)
        top = jnp.max(scores, axis=-1, keepdims=True)
        probs = jnp.where(visible, jnp.exp(scores - top), 0.0)
        denom = jnp.sum(probs, axis=-1)
        rounded = lax.optimization_barrier(probs.astype(jnp.bfloat16)).astype(jnp.float32)
        numer = jnp.einsum("kgqp,pkd->kgqd", rounded, value_matrix)
        result = numer / denom[..., None]
        result = jnp.transpose(result, (2, 0, 1, 3)).reshape(rows_per_block, QUERY_HEAD_COUNT * HEAD_WIDTH)
        return result.astype(jnp.bfloat16)

    blocks = lax.map(one_block, jnp.arange(N_CTX, dtype=jnp.int32))
    return blocks.reshape(PACKED_TOKENS, QUERY_HEAD_COUNT * HEAD_WIDTH)
```

```python
import jax
import jax.numpy as jnp
from jax import lax
from jax.experimental import pallas as pl
from jax.experimental.pallas import tpu as pltpu
from jax.sharding import Mesh, PartitionSpec as P


QUERY_HEAD_COUNT = 64
KEY_VALUE_HEADS = 8
HEAD_WIDTH = 128
GROUP = QUERY_HEAD_COUNT // KEY_VALUE_HEADS
ROW = 4
REACH = 8
HIDDEN = -1e30
EXP2_SCALE = HEAD_WIDTH ** (-0.5) * 1.4426950408889634
NT = (((1,), (1,)), ((), ()))


def doc_begin(positions, doc_starts):
    found = jnp.where(doc_starts[None, :] <= positions[:, None], doc_starts[None, :], 0)
    return jnp.max(found, axis=1)


def in_hbm(*arrays):
    return tuple(pltpu.with_memory_space_constraint(a, pltpu.HBM) for a in arrays)


def join_kernel(key_ref, value_ref, pair_ref, sem):
    tokens = key_ref.shape[0]
    copies = [
        pltpu.make_async_copy(key_ref, pair_ref.at[:tokens], sem.at[0]),
        pltpu.make_async_copy(value_ref, pair_ref.at[tokens:], sem.at[1]),
    ]
    for copy in copies:
        copy.start()
    for copy in copies:
        copy.wait()


def join(keys, values):
    anywhere, vmem = pl.BlockSpec(memory_space=pl.ANY), pl.BlockSpec(memory_space=pltpu.VMEM)
    return pl.pallas_call(
        join_kernel,
        out_shape=jax.ShapeDtypeStruct((2 * keys.shape[0], keys.shape[1]), keys.dtype),
        in_specs=[anywhere, anywhere],
        out_specs=vmem,
        scratch_shapes=[pltpu.SemaphoreType.DMA((2,))],
        compiler_params=pltpu.CompilerParams(vmem_limit_bytes=2 * 2**20),
        name="join",
    )(*in_hbm(keys, values))


def halve_kernel(query_ref, kept_ref, given_ref, sem):
    core = lax.axis_index("core")
    chips, _, width = kept_ref.shape
    copies = []
    for y in range(chips):
        for part, (into, owner) in enumerate(((kept_ref, core), (given_ref, 1 - core))):
            start = pl.multiple_of((2 * y + owner) * width, width)
            source = query_ref.at[:, pl.ds(start, width)]
            copies.append(pltpu.make_async_copy(source, into.at[y], sem.at[part, y]))
    for copy in copies:
        copy.start()
    for copy in copies:
        copy.wait()


def halve(queries, chips):
    anywhere, vmem = pl.BlockSpec(memory_space=pl.ANY), pl.BlockSpec(memory_space=pltpu.VMEM)
    half = jax.ShapeDtypeStruct((chips, queries.shape[0], GROUP * HEAD_WIDTH), queries.dtype)
    return pl.pallas_call(
        halve_kernel,
        out_shape=(half, half),
        in_specs=[anywhere],
        out_specs=(vmem, vmem),
        scratch_shapes=[pltpu.SemaphoreType.DMA((2, chips))],
        compiler_params=pltpu.CompilerParams(vmem_limit_bytes=4 * 2**20),
        name="halve",
    )(*in_hbm(queries))


def turn_kernel(kept_ref, other_ref, *out_refs):
    core, y = lax.axis_index("core"), lax.axis_index("y")
    chips, tokens, _ = kept_ref.shape
    for distance, out_ref in enumerate(out_refs):
        to = (y + distance) % chips
        out_ref[pl.ds(pl.multiple_of(core * tokens, tokens), tokens)] = kept_ref[to]
        out_ref[pl.ds(pl.multiple_of((1 - core) * tokens, tokens), tokens)] = other_ref[to]


def turn(kept, other):
    vmem = pl.BlockSpec(memory_space=pltpu.VMEM)
    chips, tokens, width = kept.shape
    return pl.pallas_call(
        turn_kernel,
        out_shape=(jax.ShapeDtypeStruct((2 * tokens, width), kept.dtype),) * chips,
        in_specs=[vmem, vmem],
        out_specs=(vmem,) * chips,
        compiler_params=pltpu.CompilerParams(vmem_limit_bytes=4 * 2**20),
        name="turn",
    )(kept, other)


def pack_kernel(own_ref, back_ref, out_ref):
    place = ROW * lax.axis_index("odd") + lax.axis_index("x")
    heads = out_ref.shape[1]
    for to in range(REACH):
        for head in range(heads):
            columns = slice(head * HEAD_WIDTH, (head + 1) * HEAD_WIDTH)
            out_ref[to, head] = jnp.where(to >= place, own_ref[:, columns], back_ref[:, columns])


def pack(own, back, heads):
    vmem = pl.BlockSpec(memory_space=pltpu.VMEM)
    return pl.pallas_call(
        pack_kernel,
        out_shape=jax.ShapeDtypeStruct((REACH, heads, own.shape[0], HEAD_WIDTH), own.dtype),
        in_specs=[vmem, vmem],
        out_specs=vmem,
        compiler_params=pltpu.CompilerParams(vmem_limit_bytes=4 * 2**20),
        name="pack",
    )(own, back)


def attend_kernel(begin_ref, *refs):
    parts, (pair_ref, out_ref, query_ref, score_a, score_b, hidden_ref) = refs[:-6], refs[-6:]
    y = lax.axis_index("y")
    for distance, part_ref in enumerate(parts):
        start = (y - distance + len(parts)) % len(parts) * part_ref.shape[0]
        query_ref[pl.ds(pl.multiple_of(start, part_ref.shape[0]), part_ref.shape[0])] = part_ref[...]
    place = ROW * lax.axis_index("odd") + lax.axis_index("x")
    block = REACH * lax.axis_index("z") + place
    rows = query_ref.shape[0]
    tile = (rows, rows)
    query_pos = block * rows + lax.broadcasted_iota(jnp.int32, tile, 0)
    lane = lax.broadcasted_iota(jnp.int32, tile, 1)
    begin = begin_ref[...]
    for j in range(REACH):
        first = block - place + jnp.where(j <= place, j, j - REACH)
        key_pos = first * rows + lane
        visible = (key_pos >= begin) & (key_pos <= query_pos)
        hidden_ref[:, j * rows : (j + 1) * rows] = jnp.where(visible, 0.0, HIDDEN)

    def scores(head, into):
        query = query_ref[:, head * HEAD_WIDTH : (head + 1) * HEAD_WIDTH]
        for j in range(REACH):
            key = pair_ref[j, :, 0].reshape(rows, HEAD_WIDTH)
            part = slice(j * rows, (j + 1) * rows)
            product = lax.dot_general(query, key, NT, preferred_element_type=jnp.float32)
            into[:, part] = product + hidden_ref[:, part]

    def output(head, score_ref):
        score = score_ref[...]
        top = jnp.max(score, axis=1, keepdims=True)
        probs = jnp.exp2((score - top) * EXP2_SCALE)
        total = jnp.sum(probs, axis=1, keepdims=True)
        probs = probs.astype(jnp.bfloat16)
        accum = jnp.zeros((rows, HEAD_WIDTH), jnp.float32)
        for j in range(REACH):
            value = pair_ref[j, :, 1].reshape(rows, HEAD_WIDTH)
            accum += jnp.dot(probs[:, j * rows : (j + 1) * rows], value, preferred_element_type=jnp.float32)
        out_ref[:, head * HEAD_WIDTH : (head + 1) * HEAD_WIDTH] = (accum / total).astype(jnp.bfloat16)

    buffers = (score_a, score_b)
    scores(0, score_a)
    for head in range(GROUP):
        if head + 1 < GROUP:
            scores(head + 1, buffers[(head + 1) % 2])
        output(head, buffers[head % 2])


def attend(begin, parts, pair):
    rows, width = begin.shape[0], parts[0].shape[1]
    vmem = pl.BlockSpec(memory_space=pltpu.VMEM)
    return pl.pallas_call(
        attend_kernel,
        out_shape=jax.ShapeDtypeStruct((rows, width), jnp.bfloat16),
        in_specs=[vmem] * (2 + len(parts)),
        out_specs=vmem,
        scratch_shapes=[pltpu.VMEM((rows, width), jnp.bfloat16)]
        + [pltpu.VMEM((rows, REACH * rows), jnp.float32)] * 3,
        compiler_params=pltpu.CompilerParams(vmem_limit_bytes=40 * 2**20),
        name="attend",
    )(begin, *parts, pair)


def body(queries, keys, values, doc_starts):
    tokens = queries.shape[0]
    n_y = lax.axis_size("y")
    n_tp = 2 * n_y
    rows = tokens * n_tp
    place = ROW * lax.axis_index("odd") + lax.axis_index("x")
    block = REACH * lax.axis_index("z") + place

    pair = join(keys, values)
    back = lax.ppermute(pair, "z", [(i, i + 1) for i in range(lax.axis_size("z") - 1)])
    sent = pack(pair, back, n_tp).reshape(REACH * n_tp, 2 * tokens, HEAD_WIDTH)
    got = lax.all_to_all(sent, ("odd", "x", "y", "core"), split_axis=0, concat_axis=0, tiled=True)
    got = got.reshape(REACH, n_tp, 2, tokens, HEAD_WIDTH)
    kept, given = halve(queries, n_y)
    other = lax.ppermute(given, "core", [(0, 1), (1, 0)])
    parts = list(turn(kept, other))
    for distance in range(1, n_y):
        route = [(i, (i + distance) % n_y) for i in range(n_y)]
        parts[distance] = lax.ppermute(parts[distance], "y", route)

    query_pos = block * rows + jnp.arange(rows, dtype=jnp.int32)
    begin = doc_begin(query_pos, doc_starts)[:, None]
    result = attend(begin, parts, got).reshape(n_tp, tokens, -1)
    return lax.all_to_all(result, ("y", "core"), split_axis=0, concat_axis=2, tiled=True)[0]


def solution(mesh):
    names = ("z", "odd", "x", "y", "core")
    split = Mesh(mesh.devices.reshape(-1, REACH // ROW, ROW, mesh.devices.shape[1] // 2, 2), names)
    whole = P(names, None)
    return jax.shard_map(body, mesh=split, in_specs=(whole, whole, whole, P()), out_specs=whole, check_vma=False)
```

```python
import functools

import jax
import jax.numpy as jnp
from jax import lax
from jax.experimental import pallas as pl
from jax.experimental.pallas import tpu as pltpu
from jax.sharding import Mesh, PartitionSpec as P


QUERY_HEAD_COUNT = 64
KEY_VALUE_HEADS = 8
HEAD_WIDTH = 128
GROUP = QUERY_HEAD_COUNT // KEY_VALUE_HEADS
ROW = 4
REACH = 8
HIDDEN = -1e30
REACHES = (4, 6, 8)
EARLY, LATE = (0, 2), (1, 3)
EXP2_SCALE = HEAD_WIDTH ** (-0.5) * 1.4426950408889634
NT = (((1,), (1,)), ((), ()))


def doc_begin(positions, doc_starts):
    found = jnp.where(doc_starts[None, :] <= positions[:, None], doc_starts[None, :], 0)
    return jnp.max(found, axis=1)


def in_hbm(*arrays):
    return tuple(pltpu.with_memory_space_constraint(a, pltpu.HBM) for a in arrays)


def join_kernel(key_ref, value_ref, pair_ref, sem):
    tokens = key_ref.shape[0]
    copies = [
        pltpu.make_async_copy(key_ref, pair_ref.at[:tokens], sem.at[0]),
        pltpu.make_async_copy(value_ref, pair_ref.at[tokens:], sem.at[1]),
    ]
    for copy in copies:
        copy.start()
    for copy in copies:
        copy.wait()


def join(keys, values):
    anywhere, vmem = pl.BlockSpec(memory_space=pl.ANY), pl.BlockSpec(memory_space=pltpu.VMEM)
    return pl.pallas_call(
        join_kernel,
        out_shape=jax.ShapeDtypeStruct((2 * keys.shape[0], keys.shape[1]), keys.dtype),
        in_specs=[anywhere, anywhere],
        out_specs=vmem,
        scratch_shapes=[pltpu.SemaphoreType.DMA((2,))],
        compiler_params=pltpu.CompilerParams(vmem_limit_bytes=2 * 2**20),
        name="join",
    )(*in_hbm(keys, values))


def halve_kernel(query_ref, kept_ref, given_ref, sem):
    core = lax.axis_index("core")
    chips, _, width = kept_ref.shape
    copies = []
    for y in range(chips):
        for part, (into, owner) in enumerate(((kept_ref, core), (given_ref, 1 - core))):
            start = pl.multiple_of((2 * y + owner) * width, width)
            source = query_ref.at[:, pl.ds(start, width)]
            copies.append(pltpu.make_async_copy(source, into.at[y], sem.at[part, y]))
    for copy in copies:
        copy.start()
    for copy in copies:
        copy.wait()


def halve(queries, chips):
    anywhere, vmem = pl.BlockSpec(memory_space=pl.ANY), pl.BlockSpec(memory_space=pltpu.VMEM)
    half = jax.ShapeDtypeStruct((chips, queries.shape[0], GROUP * HEAD_WIDTH), queries.dtype)
    return pl.pallas_call(
        halve_kernel,
        out_shape=(half, half),
        in_specs=[anywhere],
        out_specs=(vmem, vmem),
        scratch_shapes=[pltpu.SemaphoreType.DMA((2, chips))],
        compiler_params=pltpu.CompilerParams(vmem_limit_bytes=4 * 2**20),
        name="halve",
    )(*in_hbm(queries))


def turn_kernel(kept_ref, other_ref, *out_refs):
    core, y = lax.axis_index("core"), lax.axis_index("y")
    chips, tokens, _ = kept_ref.shape
    for distance, out_ref in enumerate(out_refs):
        to = (y + distance) % chips
        out_ref[pl.ds(pl.multiple_of(core * tokens, tokens), tokens)] = kept_ref[to]
        out_ref[pl.ds(pl.multiple_of((1 - core) * tokens, tokens), tokens)] = other_ref[to]


def turn(kept, other):
    vmem = pl.BlockSpec(memory_space=pltpu.VMEM)
    chips, tokens, width = kept.shape
    return pl.pallas_call(
        turn_kernel,
        out_shape=(jax.ShapeDtypeStruct((2 * tokens, width), kept.dtype),) * chips,
        in_specs=[vmem, vmem],
        out_specs=(vmem,) * chips,
        compiler_params=pltpu.CompilerParams(vmem_limit_bytes=4 * 2**20),
        name="turn",
    )(kept, other)


def pack_kernel(own_ref, back_ref, out_ref):
    place = ROW * lax.axis_index("odd") + lax.axis_index("x")
    heads = out_ref.shape[1]
    for to in range(REACH):
        for head in range(heads):
            columns = slice(head * HEAD_WIDTH, (head + 1) * HEAD_WIDTH)
            out_ref[to, head] = jnp.where(to >= place, own_ref[:, columns], back_ref[:, columns])


def pack(own, back, heads):
    vmem = pl.BlockSpec(memory_space=pltpu.VMEM)
    return pl.pallas_call(
        pack_kernel,
        out_shape=jax.ShapeDtypeStruct((REACH, heads, own.shape[0], HEAD_WIDTH), own.dtype),
        in_specs=[vmem, vmem],
        out_specs=vmem,
        compiler_params=pltpu.CompilerParams(vmem_limit_bytes=4 * 2**20),
        name="pack",
    )(own, back)


def attend_kernel(distances, need_ref, begin_ref, *refs):
    count = len(distances)
    parts, (pair_ref, *done_refs, out_ref, query_ref, score_a, score_b, hidden_ref) = refs[:count], refs[count:]
    y = lax.axis_index("y")
    chips = lax.axis_size("y")
    chunk = parts[0].shape[0]
    rows, keys = query_ref.shape[0], score_a.shape[1] // REACH

    def offset(distance):
        return pl.multiple_of((y - distance + chips) % chips * chunk, chunk)

    place = ROW * lax.axis_index("odd") + lax.axis_index("x")
    block = REACH * lax.axis_index("z") + place
    for i, part_ref in enumerate(parts):
        query_ref[i * chunk : (i + 1) * chunk] = part_ref[...]
    if done_refs:
        for i, distance in enumerate(EARLY):
            out_ref[pl.ds(offset(distance), chunk)] = done_refs[0][i * chunk : (i + 1) * chunk]

    def over(reach):
        if reach == REACH:
            slots = list(range(REACH))
            blocks = [block - place + jnp.where(j <= place, j, j - REACH) for j in slots]
        else:
            slots = [(place + REACH - reach + 1 + j) % REACH for j in range(reach)]
            blocks = [block - reach + 1 + j for j in range(reach)]
        lane = lax.broadcasted_iota(jnp.int32, (chunk, keys), 1)
        for i, distance in enumerate(distances):
            begin = begin_ref[pl.ds(offset(distance), chunk)]
            query_pos = block * keys + offset(distance) + lax.broadcasted_iota(jnp.int32, (chunk, keys), 0)
            for j in range(reach):
                key_pos = blocks[j] * keys + lane
                visible = (key_pos >= begin) & (key_pos <= query_pos)
                hidden_ref[i * chunk : (i + 1) * chunk, j * keys : (j + 1) * keys] = jnp.where(visible, 0.0, HIDDEN)

        def scores(head, into):
            query = query_ref[:, head * HEAD_WIDTH : (head + 1) * HEAD_WIDTH]
            for j in range(reach):
                key = pair_ref[slots[j], :, 0].reshape(keys, HEAD_WIDTH)
                part = slice(j * keys, (j + 1) * keys)
                product = lax.dot_general(query, key, NT, preferred_element_type=jnp.float32)
                into[:, part] = product + hidden_ref[:, part]

        def output(head, score_ref):
            score = score_ref[:, : reach * keys]
            top = jnp.max(score, axis=1, keepdims=True)
            probs = jnp.exp2((score - top) * EXP2_SCALE)
            total = jnp.sum(probs, axis=1, keepdims=True)
            probs = probs.astype(jnp.bfloat16)
            accum = jnp.zeros((rows, HEAD_WIDTH), jnp.float32)
            for j in range(reach):
                value = pair_ref[slots[j], :, 1].reshape(keys, HEAD_WIDTH)
                accum += jnp.dot(probs[:, j * keys : (j + 1) * keys], value, preferred_element_type=jnp.float32)
            result = (accum / total).astype(jnp.bfloat16)
            columns = slice(head * HEAD_WIDTH, (head + 1) * HEAD_WIDTH)
            if out_ref.shape[0] == rows:
                out_ref[:, columns] = result
            else:
                for i, distance in enumerate(distances):
                    out_ref[pl.ds(offset(distance), chunk), columns] = result[i * chunk : (i + 1) * chunk]

        buffers = (score_a, score_b)
        scores(0, score_a)
        for head in range(GROUP):
            if head + 1 < GROUP:
                scores(head + 1, buffers[(head + 1) % 2])
            output(head, buffers[head % 2])

    need = need_ref[0]
    for less, reach in zip((0,) + REACHES, REACHES):
        pl.when((need > less) & (need <= reach))(functools.partial(over, reach))


def attend(distances, need, begin, parts, pair, *done):
    keys, width = begin.shape[0], parts[0].shape[1]
    rows = len(parts) * parts[0].shape[0]
    vmem = pl.BlockSpec(memory_space=pltpu.VMEM)
    return pl.pallas_call(
        functools.partial(attend_kernel, distances),
        out_shape=jax.ShapeDtypeStruct((keys if done else rows, width), jnp.bfloat16),
        in_specs=[pl.BlockSpec(memory_space=pltpu.SMEM)] + [vmem] * (2 + len(parts) + len(done)),
        out_specs=vmem,
        scratch_shapes=[pltpu.VMEM((rows, width), jnp.bfloat16)]
        + [pltpu.VMEM((rows, REACH * keys), jnp.float32)] * 3,
        compiler_params=pltpu.CompilerParams(vmem_limit_bytes=20 * 2**20),
        name="attend",
    )(need, begin, *parts, pair, *done)


def body(queries, keys, values, doc_starts):
    tokens = queries.shape[0]
    n_y = lax.axis_size("y")
    n_tp = 2 * n_y
    rows = tokens * n_tp
    place = ROW * lax.axis_index("odd") + lax.axis_index("x")
    block = REACH * lax.axis_index("z") + place

    pair = join(keys, values)
    back = lax.ppermute(pair, "z", [(i, i + 1) for i in range(lax.axis_size("z") - 1)])
    sent = pack(pair, back, n_tp).reshape(REACH * n_tp, 2 * tokens, HEAD_WIDTH)
    got = lax.all_to_all(sent, ("odd", "x", "y", "core"), split_axis=0, concat_axis=0, tiled=True)
    got = got.reshape(REACH, n_tp, 2, tokens, HEAD_WIDTH)
    kept, given = halve(queries, n_y)
    other = lax.ppermute(given, "core", [(0, 1), (1, 0)])
    parts = list(turn(kept, other))
    for distance in range(1, n_y):
        route = [(i, (i + distance) % n_y) for i in range(n_y)]
        parts[distance] = lax.ppermute(parts[distance], "y", route)

    query_pos = block * rows + jnp.arange(rows, dtype=jnp.int32)
    begin = doc_begin(query_pos, doc_starts)
    need = block + 1 - begin[:1] // rows
    begin = begin[:, None]
    early = attend(EARLY, need, begin, [parts[d] for d in EARLY], got)
    result = attend(LATE, need, begin, [parts[d] for d in LATE], got, early)
    result = result.reshape(n_tp, tokens, -1)
    return lax.all_to_all(result, ("y", "core"), split_axis=0, concat_axis=2, tiled=True)[0]


def solution(mesh):
    names = ("z", "odd", "x", "y", "core")
    split = Mesh(mesh.devices.reshape(-1, REACH // ROW, ROW, mesh.devices.shape[1] // 2, 2), names)
    whole = P(names, None)
    return jax.shard_map(body, mesh=split, in_specs=(whole, whole, whole, P()), out_specs=whole, check_vma=False)
```

```python
import functools

import jax
import jax.numpy as jnp
from jax import lax
from jax.experimental import pallas as pl
from jax.experimental.pallas import tpu as pltpu
from jax.sharding import Mesh, PartitionSpec as P


QUERY_HEAD_COUNT = 64
KEY_VALUE_HEADS = 8
HEAD_WIDTH = 128
GROUP = QUERY_HEAD_COUNT // KEY_VALUE_HEADS
ROW = 4
REACH = 8
HIDDEN = -1e30
ORDER = ("y", "core", "odd", "x")
REACHES = (4, 6, 8)
EARLY, LATE = (0, 2), (1, 3)
EXP2_SCALE = HEAD_WIDTH ** (-0.5) * 1.4426950408889634
NT = (((1,), (1,)), ((), ()))


def doc_begin(positions, doc_starts):
    found = jnp.where(doc_starts[None, :] <= positions[:, None], doc_starts[None, :], 0)
    return jnp.max(found, axis=1)


def in_hbm(*arrays):
    return tuple(pltpu.with_memory_space_constraint(a, pltpu.HBM) for a in arrays)


def join_kernel(key_ref, value_ref, pair_ref, sem):
    tokens = key_ref.shape[0]
    copies = [
        pltpu.make_async_copy(key_ref, pair_ref.at[:tokens], sem.at[0]),
        pltpu.make_async_copy(value_ref, pair_ref.at[tokens:], sem.at[1]),
    ]
    for copy in copies:
        copy.start()
    for copy in copies:
        copy.wait()


def join(keys, values):
    anywhere, vmem = pl.BlockSpec(memory_space=pl.ANY), pl.BlockSpec(memory_space=pltpu.VMEM)
    return pl.pallas_call(
        join_kernel,
        out_shape=jax.ShapeDtypeStruct((2 * keys.shape[0], keys.shape[1]), keys.dtype),
        in_specs=[anywhere, anywhere],
        out_specs=vmem,
        scratch_shapes=[pltpu.SemaphoreType.DMA((2,))],
        compiler_params=pltpu.CompilerParams(vmem_limit_bytes=2 * 2**20),
        name="join",
    )(*in_hbm(keys, values))


def halve_kernel(query_ref, kept_ref, given_ref, sem):
    core = lax.axis_index("core")
    chips, _, width = kept_ref.shape
    copies = []
    for y in range(chips):
        for part, (into, owner) in enumerate(((kept_ref, core), (given_ref, 1 - core))):
            start = pl.multiple_of((2 * y + owner) * width, width)
            source = query_ref.at[:, pl.ds(start, width)]
            copies.append(pltpu.make_async_copy(source, into.at[y], sem.at[part, y]))
    for copy in copies:
        copy.start()
    for copy in copies:
        copy.wait()


def halve(queries, chips):
    anywhere, vmem = pl.BlockSpec(memory_space=pl.ANY), pl.BlockSpec(memory_space=pltpu.VMEM)
    half = jax.ShapeDtypeStruct((chips, queries.shape[0], GROUP * HEAD_WIDTH), queries.dtype)
    return pl.pallas_call(
        halve_kernel,
        out_shape=(half, half),
        in_specs=[anywhere],
        out_specs=(vmem, vmem),
        scratch_shapes=[pltpu.SemaphoreType.DMA((2, chips))],
        compiler_params=pltpu.CompilerParams(vmem_limit_bytes=4 * 2**20),
        name="halve",
    )(*in_hbm(queries))


def turn_kernel(kept_ref, other_ref, *out_refs):
    core, y = lax.axis_index("core"), lax.axis_index("y")
    chips, tokens, _ = kept_ref.shape
    for distance, out_ref in enumerate(out_refs):
        to = (y + distance) % chips
        out_ref[pl.ds(pl.multiple_of(core * tokens, tokens), tokens)] = kept_ref[to]
        out_ref[pl.ds(pl.multiple_of((1 - core) * tokens, tokens), tokens)] = other_ref[to]


def turn(kept, other):
    vmem = pl.BlockSpec(memory_space=pltpu.VMEM)
    chips, tokens, width = kept.shape
    return pl.pallas_call(
        turn_kernel,
        out_shape=(jax.ShapeDtypeStruct((2 * tokens, width), kept.dtype),) * chips,
        in_specs=[vmem, vmem],
        out_specs=(vmem,) * chips,
        compiler_params=pltpu.CompilerParams(vmem_limit_bytes=4 * 2**20),
        name="turn",
    )(kept, other)


def peer(place, head):
    sizes = {"odd": REACH // ROW, "x": ROW, "y": KEY_VALUE_HEADS // 2, "core": 2}
    at = {"odd": place // ROW, "x": place % ROW, "y": head // 2, "core": head % 2}
    index = 0
    for axis in ORDER:
        index = index * sizes[axis] + at[axis]
    return index


def pack_kernel(own_ref, back_ref, out_ref):
    place = ROW * lax.axis_index("odd") + lax.axis_index("x")
    heads = out_ref.shape[0] // REACH
    for to in range(REACH):
        for head in range(heads):
            columns = slice(head * HEAD_WIDTH, (head + 1) * HEAD_WIDTH)
            out_ref[peer(to, head)] = jnp.where(to >= place, own_ref[:, columns], back_ref[:, columns])


def pack(own, back, heads):
    vmem = pl.BlockSpec(memory_space=pltpu.VMEM)
    return pl.pallas_call(
        pack_kernel,
        out_shape=jax.ShapeDtypeStruct((REACH * heads, own.shape[0], HEAD_WIDTH), own.dtype),
        in_specs=[vmem, vmem],
        out_specs=vmem,
        compiler_params=pltpu.CompilerParams(vmem_limit_bytes=4 * 2**20),
        name="pack",
    )(own, back)


def attend_kernel(distances, need_ref, begin_ref, *refs):
    count = len(distances)
    parts, (pair_ref, *done_refs, out_ref, query_ref, score_a, score_b, hidden_ref) = refs[:count], refs[count:]
    y = lax.axis_index("y")
    chips = lax.axis_size("y")
    chunk = parts[0].shape[0]
    rows, keys = query_ref.shape[0], score_a.shape[1] // REACH

    def offset(distance):
        return pl.multiple_of((y - distance + chips) % chips * chunk, chunk)

    place = ROW * lax.axis_index("odd") + lax.axis_index("x")
    block = REACH * lax.axis_index("z") + place
    for i, part_ref in enumerate(parts):
        query_ref[i * chunk : (i + 1) * chunk] = part_ref[...]
    if done_refs:
        for i, distance in enumerate(EARLY):
            out_ref[pl.ds(offset(distance), chunk)] = done_refs[0][i * chunk : (i + 1) * chunk]

    def gathered(slot, which):
        pieces = [pair_ref[peer(slot, piece), which] for piece in range(KEY_VALUE_HEADS)]
        return jnp.concatenate(pieces, axis=0)

    def over(reach):
        if reach == REACH:
            slots = list(range(REACH))
            blocks = [block - place + jnp.where(j <= place, j, j - REACH) for j in slots]
        else:
            slots = [(place + REACH - reach + 1 + j) % REACH for j in range(reach)]
            blocks = [block - reach + 1 + j for j in range(reach)]
        lane = lax.broadcasted_iota(jnp.int32, (chunk, keys), 1)
        for i, distance in enumerate(distances):
            begin = begin_ref[pl.ds(offset(distance), chunk)]
            query_pos = block * keys + offset(distance) + lax.broadcasted_iota(jnp.int32, (chunk, keys), 0)
            for j in range(reach):
                key_pos = blocks[j] * keys + lane
                visible = (key_pos >= begin) & (key_pos <= query_pos)
                hidden_ref[i * chunk : (i + 1) * chunk, j * keys : (j + 1) * keys] = jnp.where(visible, 0.0, HIDDEN)

        def scores(head, into):
            query = query_ref[:, head * HEAD_WIDTH : (head + 1) * HEAD_WIDTH]
            for j in range(reach):
                key = gathered(slots[j], 0)
                part = slice(j * keys, (j + 1) * keys)
                product = lax.dot_general(query, key, NT, preferred_element_type=jnp.float32)
                into[:, part] = product + hidden_ref[:, part]

        def output(head, score_ref):
            score = score_ref[:, : reach * keys]
            top = jnp.max(score, axis=1, keepdims=True)
            probs = jnp.exp2((score - top) * EXP2_SCALE)
            total = jnp.sum(probs, axis=1, keepdims=True)
            probs = probs.astype(jnp.bfloat16)
            accum = jnp.zeros((rows, HEAD_WIDTH), jnp.float32)
            for j in range(reach):
                value = gathered(slots[j], 1)
                accum += jnp.dot(probs[:, j * keys : (j + 1) * keys], value, preferred_element_type=jnp.float32)
            result = (accum / total).astype(jnp.bfloat16)
            columns = slice(head * HEAD_WIDTH, (head + 1) * HEAD_WIDTH)
            if out_ref.shape[0] == rows:
                out_ref[:, columns] = result
            else:
                for i, distance in enumerate(distances):
                    out_ref[pl.ds(offset(distance), chunk), columns] = result[i * chunk : (i + 1) * chunk]

        buffers = (score_a, score_b)
        scores(0, score_a)
        for head in range(GROUP):
            if head + 1 < GROUP:
                scores(head + 1, buffers[(head + 1) % 2])
            output(head, buffers[head % 2])

    need = need_ref[0]
    for less, reach in zip((0,) + REACHES, REACHES):
        pl.when((need > less) & (need <= reach))(functools.partial(over, reach))


def attend(distances, need, begin, parts, pair, *done):
    keys, width = begin.shape[0], parts[0].shape[1]
    rows = len(parts) * parts[0].shape[0]
    vmem = pl.BlockSpec(memory_space=pltpu.VMEM)
    return pl.pallas_call(
        functools.partial(attend_kernel, distances),
        out_shape=jax.ShapeDtypeStruct((keys if done else rows, width), jnp.bfloat16),
        in_specs=[pl.BlockSpec(memory_space=pltpu.SMEM)] + [vmem] * (2 + len(parts) + len(done)),
        out_specs=vmem,
        scratch_shapes=[pltpu.VMEM((rows, width), jnp.bfloat16)]
        + [pltpu.VMEM((rows, REACH * keys), jnp.float32)] * 3,
        compiler_params=pltpu.CompilerParams(vmem_limit_bytes=20 * 2**20),
        name="attend",
    )(need, begin, *parts, pair, *done)


def body(queries, keys, values, doc_starts):
    tokens = queries.shape[0]
    n_y = lax.axis_size("y")
    n_tp = 2 * n_y
    rows = tokens * n_tp
    place = ROW * lax.axis_index("odd") + lax.axis_index("x")
    block = REACH * lax.axis_index("z") + place

    pair = join(keys, values)
    back = lax.ppermute(pair, "z", [(i, i + 1) for i in range(lax.axis_size("z") - 1)])
    sent = pack(pair, back, n_tp)
    got = lax.all_to_all(sent, ORDER, split_axis=0, concat_axis=0, tiled=True)
    got = got.reshape(REACH * n_tp, 2, tokens, HEAD_WIDTH)
    kept, given = halve(queries, n_y)
    other = lax.ppermute(given, "core", [(0, 1), (1, 0)])
    parts = list(turn(kept, other))
    for distance in range(1, n_y):
        route = [(i, (i + distance) % n_y) for i in range(n_y)]
        parts[distance] = lax.ppermute(parts[distance], "y", route)

    query_pos = block * rows + jnp.arange(rows, dtype=jnp.int32)
    begin = doc_begin(query_pos, doc_starts)
    need = jnp.minimum(block + 1 - begin[:1] // rows, REACH)
    begin = begin[:, None]
    early = attend(EARLY, need, begin, [parts[d] for d in EARLY], got)
    result = attend(LATE, need, begin, [parts[d] for d in LATE], got, early)
    result = result.reshape(n_tp, tokens, -1)
    return lax.all_to_all(result, ("y", "core"), split_axis=0, concat_axis=2, tiled=True)[0]


def solution(mesh):
    names = ("z", "odd", "x", "y", "core")
    split = Mesh(mesh.devices.reshape(-1, REACH // ROW, ROW, mesh.devices.shape[1] // 2, 2), names)
    whole = P(names, None)
    return jax.shard_map(body, mesh=split, in_specs=(whole, whole, whole, P()), out_specs=whole, check_vma=False)
```
